512 devices in a mesh: groups: 2 (over y), band: 64 (over z, core), chan: 4 (over x).
Axes of the slice: x: 4, y: 2, z: 32, core: 2. Of those that a mesh axis runs over, the one named last changes fastest.
The devices are a block of a 4x16x32 slice.
Arguments:
- slide_region: float32 [16, 512, 8192], P('chan', ('groups', 'band')), parts along dimension 1, may hold values from -6 to 6
- row_taps: float32 [16, 257], P('chan'), may hold values from -0.375 to 0.375
- column_taps: float32 [16, 257], replicated, may hold values from -0.375 to 0.375
- channel_mix: float32 [16, 16], replicated, may hold values from -1.5 to 1.5
Outputs:
- filtered: float32 [16, 512, 8192], P('chan', ('groups', 'band')), parts along dimension 1
The draws below stay inside these ranges and needn't reach their ends.
There are 2 independent parts, one for each index of `groups`. The reference program is written for one: setup_inputs(seed, part) draws one part's arguments, and reference() takes and returns one part's arrays. A program takes and returns all parts, laid end to end along the dimension named above; an argument that names none is the same for every part. Nothing has to cross between parts.
All inputs are finite; a program needn't handle non-finite values.
Results may differ from the reference program's by a relative error of at most 0.00007.
Values sent between devices are 32-bit elements; how exact they have to be, the bound alone decides.
No kernel may reach another device: no remote copies, remote signals or barrier semaphores. Data moves between devices by JAX's collectives and lax.ppermute only.
A program may use at most 64 MiB of HBM per device.

```python
import jax
import jax.numpy as jnp
from jax import lax

C = 16
TAPS = 257
COLS = 8192
ROWS = 256


def block_scale(own_key, shape, split, least, largest):
    loudness, own = 1.0, jax.random.fold_in(own_key, 6)
    for axis_at, shards_of in split:
        draws = jnp.exp(jax.random.uniform(jax.random.fold_in(own, axis_at), (shards_of,), jnp.float32, least / len(split), largest / len(split)))
        loudness = loudness * jnp.repeat(draws, shape[axis_at] // shards_of).reshape([-1 if axis == axis_at else 1 for axis in range(len(shape))])
    return loudness


def scatter_about(own_key, shape, spread, reach, shards=(), dtype=jnp.bfloat16):
    loudness = block_scale(own_key, shape, shards, -0.22, 0.18) if shards else 1.0
    drawn = jax.random.normal(own_key, shape, jnp.float32) * spread * loudness
    return jnp.minimum(jnp.maximum(drawn, -reach), reach).astype(dtype)


def setup_inputs(seed: int = 0, part: int = 0) -> dict:
    arg_keys = jax.random.split(jax.random.key(seed), 5)
    part_splits = jax.random.split(jax.random.fold_in(arg_keys[4], part), 5)
    slide_region = scatter_about(part_splits[0], (C, ROWS, COLS), 1.0, 6.0, ((0, 4), (1, 64)), jnp.float32)
    row_taps = scatter_about(arg_keys[1], (C, TAPS), TAPS ** -0.5, 0.375, ((0, 4),), jnp.float32)
    column_taps = scatter_about(arg_keys[2], (C, TAPS), TAPS ** -0.5, 0.375, (), jnp.float32)
    channel_mix = scatter_about(arg_keys[3], (C, C), C ** -0.5, 1.5, (), jnp.float32)
    return dict(slide_region=slide_region, row_taps=row_taps, column_taps=column_taps, channel_mix=channel_mix)


def depthwise(signal, filter_taps, horizontal):
    channels = signal.shape[0]
    margin = (filter_taps.shape[1] - 1) // 2
    if horizontal:
        kernel = filter_taps[:, None, None, :]
        padding = ((0, 0), (margin, margin))
    else:
        kernel = filter_taps[:, None, :, None]
        padding = ((margin, margin), (0, 0))
    result = lax.conv_general_dilated(signal[None], kernel, (1, 1), padding,
                                      dimension_numbers=("NCHW", "OIHW", "NCHW"),
                                      feature_group_count=channels,
                                      precision=lax.Precision.HIGHEST)
    return result[0]


def reference(slide_region, row_taps, column_taps, channel_mix):
    across = depthwise(slide_region, row_taps, True)
    vertical = depthwise(across, column_taps, False)
    return jnp.einsum("oc,chw->ohw", channel_mix, vertical, precision=lax.Precision.HIGHEST)
```

```python
import jax
import jax.numpy as jnp
from jax import lax
from jax.experimental import pallas as pl
from jax.experimental.pallas import tpu as pltpu
from jax.sharding import Mesh
from jax.sharding import PartitionSpec as P

BAND = ("band_0", "band_1")
GROUPS_BAND = ("groups", "band_0", "band_1")
EVERYONE = ("band_0", "band_1", "chan")
LANES = 128


def dot(a, b, dims):
    return lax.dot_general(
        a, b, (dims, ((), ())), precision=lax.Precision.HIGHEST, preferred_element_type=jnp.float32
    )


def lane_block(shape, width):
    return lax.broadcasted_iota(jnp.int32, shape, len(shape) - 1) // width


def blocks_transposed(parts):
    n = len(parts)
    width = LANES // n
    which = lane_block(parts[0].shape, width)
    out = []
    for b in range(n):
        total = None
        for a in range(n):
            shift = (width * (a - b)) % LANES
            moved = pltpu.roll(parts[a], shift, axis=1) if shift else parts[a]
            total = moved if total is None else jnp.where(which == a, moved, total)
        out.append(total)
    return out


def shifted_copies(taps_row, rows, size, first):
    wide = jnp.broadcast_to(taps_row, (rows, size))
    return pltpu.roll(wide, first % size, axis=1, stride=1, stride_axis=0)


def across_kernel(x_ref, taps_ref, out_ref, padded_ref, strip_ref):
    channels, rows, cols = x_ref.shape
    tiles = cols // LANES
    length = taps_ref.shape[1]
    padded_ref[...] = jnp.zeros(padded_ref.shape, jnp.float32)
    padded_ref[:, 0:length] = taps_ref[...]
    body = rows * tiles
    edge = jnp.zeros((rows, LANES), jnp.float32)
    filtered = []
    for c in range(channels):
        strip_ref[c, 0:rows, :] = edge
        strip_ref[c, body + rows : body + 2 * rows, :] = edge
        for t in range(tiles):
            strip_ref[c, rows * (t + 1) : rows * (t + 2), :] = x_ref[c, :, LANES * t : LANES * (t + 1)]
        table = shifted_copies(padded_ref[c : c + 1, :], LANES, padded_ref.shape[1], 0)
        total = None
        for k in range(3):
            part = dot(
                strip_ref[c, rows * k : rows * k + body, :],
                table[:, LANES * k : LANES * (k + 1)],
                ((1,), (1,)),
            )
            total = part if total is None else total + part
        filtered.append(total)
    packed = blocks_transposed(filtered)
    for q, value in enumerate(packed):
        for t in range(tiles):
            at = rows * (len(packed) * t + q)
            out_ref[at : at + rows, :] = value[rows * t : rows * (t + 1), :]


def tables_kernel(taps_ref, mix_ref, table_ref, wide_mix_ref, padded_ref):
    channels, length = taps_ref.shape
    size = table_ref.shape[1]
    margin = (length - 1) // 2
    padded_ref[...] = jnp.zeros(padded_ref.shape, jnp.float32)
    padded_ref[:, 0:length] = taps_ref[...]
    for c in range(channels):
        rolled = shifted_copies(padded_ref[c : c + 1, :], size, padded_ref.shape[1], -margin)
        table_ref[c] = rolled[:, 0:size]
    n = wide_mix_ref.shape[0]
    width = n // channels
    spread = (
        lax.broadcasted_iota(jnp.int32, (n, channels), 0) // width
        == lax.broadcasted_iota(jnp.int32, (n, channels), 1)
    ).astype(jnp.float32)
    tall = dot(spread, mix_ref[...], ((1,), (1,)))
    wide = dot(tall, spread, ((1,), (1,)))
    same = (
        lax.broadcasted_iota(jnp.int32, (n, n), 0) % width
        == lax.broadcasted_iota(jnp.int32, (n, n), 1) % width
    )
    wide_mix_ref[...] = jnp.where(same, wide, 0.0)


def vertical_kernel(in_ref, table_ref, wide_mix_ref, out_ref, gathered_ref, vertical_ref):
    height = gathered_ref.shape[1]
    quarters = gathered_ref.shape[0]
    sources = in_ref.shape[0] // (quarters * 4)
    rows = height // sources
    per = table_ref.shape[0] // quarters
    which = lane_block((height, LANES), LANES // per)
    for x in range(quarters):
        for s in range(sources):
            at = rows * (quarters * s + x)
            gathered_ref[x, rows * s : rows * (s + 1), :] = in_ref[at : at + rows, :]
        mine = gathered_ref[x]
        total = None
        for c in range(per):
            part = dot(table_ref[per * x + c], jnp.where(which == c, mine, 0.0), ((1,), (0,)))
            total = part if total is None else total + part
        vertical_ref[:, LANES * x : LANES * (x + 1)] = total
    mixed = dot(vertical_ref[...], wide_mix_ref[...], ((1,), (0,)))
    for x in range(quarters):
        for s in range(sources):
            at = rows * (quarters * s + x)
            out_ref[at : at + rows, :] = mixed[rows * s : rows * (s + 1), LANES * x : LANES * (x + 1)]


def unpack_kernel(in_ref, out_ref, strip_ref):
    channels, rows, cols = out_ref.shape
    tiles = cols // LANES
    quarters = strip_ref.shape[0]
    for q in range(quarters):
        for t in range(tiles):
            at = rows * (quarters * t + q)
            strip_ref[q, rows * t : rows * (t + 1), :] = in_ref[at : at + rows, :]
    joined = blocks_transposed([strip_ref[q] for q in range(quarters)])
    for o, value in enumerate(joined):
        for t in range(tiles):
            out_ref[o, :, LANES * t : LANES * (t + 1)] = value[rows * t : rows * (t + 1), :]


def on_device(slide_region, row_taps, column_taps, channel_mix):
    channels, rows, cols = slide_region.shape
    bands = lax.axis_size(BAND)
    quarters = lax.axis_size("chan")
    height = rows * bands
    everyone = bands * quarters
    all_channels = column_taps.shape[0]
    f32 = jnp.float32
    flat = jax.ShapeDtypeStruct((everyone * rows, LANES), f32)
    scratch = pltpu.VMEM

    packed = pl.pallas_call(
        across_kernel,
        out_shape=flat,
        scratch_shapes=[
            scratch((channels, 4 * LANES), f32),
            scratch((channels, rows * (cols // LANES + 2), LANES), f32),
        ],
        name="across",
    )(slide_region, row_taps)
    table, wide_mix = pl.pallas_call(
        tables_kernel,
        out_shape=(
            jax.ShapeDtypeStruct((all_channels, height, height), f32),
            jax.ShapeDtypeStruct((quarters * LANES, quarters * LANES), f32),
        ),
        scratch_shapes=[scratch((all_channels, 4 * LANES), f32)],
        name="tables",
    )(column_taps, channel_mix)

    def exchanged(value):
        parts = value.reshape(everyone, rows, LANES)
        return lax.all_to_all(parts, EVERYONE, 0, 0, tiled=True).reshape(value.shape)

    mixed = pl.pallas_call(
        vertical_kernel,
        out_shape=flat,
        scratch_shapes=[
            scratch((quarters, height, LANES), f32),
            scratch((height, quarters * LANES), f32),
        ],
        name="vertical",
    )(exchanged(packed), table, wide_mix)
    return pl.pallas_call(
        unpack_kernel,
        out_shape=jax.ShapeDtypeStruct((channels, rows, cols), f32),
        scratch_shapes=[scratch((quarters, rows * (cols // LANES), LANES), f32)],
        name="unpack",
    )(exchanged(mixed))


def solution(mesh):
    bands = mesh.shape["band"]
    split = Mesh(
        mesh.devices.reshape(mesh.shape["groups"], bands // 2, 2, mesh.shape["chan"]),
        ("groups", "band_0", "band_1", "chan"),
    )
    in_specs = (P("chan", GROUPS_BAND, None), P("chan", None), P(), P())
    out_specs = P("chan", GROUPS_BAND, None)
    return jax.shard_map(
        on_device, mesh=split, in_specs=in_specs, out_specs=out_specs, check_vma=False
    )
```

```python
import jax
import jax.numpy as jnp
from jax import lax
from jax.experimental import pallas as pl
from jax.experimental.pallas import tpu as pltpu
from jax.sharding import Mesh
from jax.sharding import PartitionSpec as P

BAND = ("band_0", "band_1")
GROUPS_BAND = ("groups", "band_0", "band_1")
EVERYONE = ("band_0", "band_1", "chan")
LANES = 128
F32 = jnp.float32
BF16 = jnp.bfloat16
IN_VMEM = pl.BlockSpec(memory_space=pltpu.VMEM)
IN_HBM = pl.BlockSpec(memory_space=pltpu.HBM)
SMALL = pltpu.CompilerParams(vmem_limit_bytes=16 * 1024 * 1024)


def halves(value):
    high = value.astype(BF16)
    return high, (value - high.astype(F32)).astype(BF16)


def dot(a, b, dims):
    return lax.dot_general(a, b, (dims, ((), ())), preferred_element_type=F32)


def dot_of_halves(a, b, dims):
    (a_high, a_low), (b_high, b_low) = a, b
    return dot(a_high, b_high, dims) + (dot(a_high, b_low, dims) + dot(a_low, b_high, dims))


def lane_block(shape, width):
    return lax.broadcasted_iota(jnp.int32, shape, len(shape) - 1) // width


def blocks_transposed(parts, wanted):
    width = LANES // len(parts)
    which = lane_block(parts[0].shape, width)
    out = []
    for b in wanted:
        total = None
        for a, part in enumerate(parts):
            shift = (width * (a - b)) % LANES
            moved = pltpu.roll(part, shift, axis=1) if shift else part
            total = moved if total is None else jnp.where(which == a, moved, total)
        out.append(total)
    return out


def shifted_copies(taps_row, rows, size, first):
    wide = jnp.broadcast_to(taps_row, (rows, size))
    return pltpu.roll(wide, first % size, axis=1, stride=1, stride_axis=0)


def across_kernel(x_hbm, taps_ref, out_ref, x_ref, padded_ref, lhs_ref, arrived):
    channels, rows, cols = x_ref.shape
    tiles = cols // LANES
    pairs = tiles // 2
    body = rows * pairs
    length = taps_ref.shape[1]
    copies = [pltpu.make_async_copy(x_hbm.at[c], x_ref.at[c], arrived.at[c]) for c in range(channels)]
    for copy in copies:
        copy.start()
    padded_ref[...] = jnp.zeros(padded_ref.shape, F32)
    padded_ref[:, 0:length] = taps_ref[...]
    edge = jnp.zeros((rows, LANES), F32)
    filtered = ([], [])
    for c in range(channels):
        table = halves(shifted_copies(padded_ref[c : c + 1, :], 2 * LANES, padded_ref.shape[1], 0))
        lhs_ref[c, 0:rows, 0:LANES] = edge
        lhs_ref[c, body - rows : body, 3 * LANES : 4 * LANES] = edge
        copies[c].wait()
        for t in range(tiles):
            tile = x_ref[c, :, LANES * t : LANES * (t + 1)]
            p, odd = t // 2, t % 2
            lhs_ref[c, rows * p : rows * (p + 1), LANES * (1 + odd) : LANES * (2 + odd)] = tile
            q = p + 1 if odd else p - 1
            if 0 <= q < pairs:
                at = 0 if odd else 3 * LANES
                lhs_ref[c, rows * q : rows * (q + 1), at : at + LANES] = tile
        total = dot_of_halves(halves(lhs_ref[c]), table, ((1,), (1,)))
        filtered[0].append(total[:, 0:LANES])
        filtered[1].append(total[:, LANES : 2 * LANES])
    for odd in range(2):
        packed = blocks_transposed(filtered[odd], range(channels))
        for q, value in enumerate(packed):
            for p in range(pairs):
                at = rows * (channels * (2 * p + odd) + q)
                out_ref[at : at + rows, :] = value[rows * p : rows * (p + 1), :]


def tables_kernel(taps_ref, mix_ref, high_ref, low_ref, wide_mix_ref, padded_ref):
    channels, length = taps_ref.shape
    quarters, half = high_ref.shape[0:2]
    margin = (length - 1) // 2
    padded_ref[...] = jnp.zeros(padded_ref.shape, F32)
    padded_ref[:, 0:length] = taps_ref[...]
    per = channels // quarters
    for c in range(channels):
        rolled = shifted_copies(padded_ref[c : c + 1, :], half, padded_ref.shape[1], half - margin)
        high, low = halves(rolled[:, 0 : 3 * half])
        at = 3 * half * (c % per)
        high_ref[c // per, :, at : at + 3 * half] = high
        low_ref[c // per, :, at : at + 3 * half] = low
    n = wide_mix_ref.shape[1]
    width = n // channels
    spread = (
        lax.broadcasted_iota(jnp.int32, (n, channels), 0) // width
        == lax.broadcasted_iota(jnp.int32, (n, channels), 1)
    ).astype(F32)
    precise = dict(precision=lax.Precision.HIGHEST, preferred_element_type=F32)
    tall = lax.dot_general(spread, mix_ref[...], (((1,), (1,)), ((), ())), **precise)
    wide = lax.dot_general(tall, spread, (((1,), (1,)), ((), ())), **precise)
    same = (
        lax.broadcasted_iota(jnp.int32, (n, n), 0) % width
        == lax.broadcasted_iota(jnp.int32, (n, n), 1) % width
    )
    wide_mix_ref[0], wide_mix_ref[1] = halves(jnp.where(same, wide, 0.0))


def vertical_kernel(
    strip, in_ref, high_ref, low_hbm, mix_hbm, out_ref, gathered_ref, vertical_ref, low_ref, mix_ref, arrived
):
    quarters, height = gathered_ref.shape[0:2]
    half = height // 2
    per = high_ref.shape[2] // (3 * half)
    sources = height // strip
    low_copy = pltpu.make_async_copy(low_hbm, low_ref, arrived.at[0])
    mix_copy = pltpu.make_async_copy(mix_hbm, mix_ref, arrived.at[1])
    low_copy.start()
    mix_copy.start()
    which = lane_block((height, LANES), LANES // per)
    masked = []
    for x in range(quarters):
        for s in range(sources):
            at = strip * (quarters * s + x)
            gathered_ref[x, strip * s : strip * (s + 1), :] = in_ref[at : at + strip, :]
        mine = gathered_ref[x]
        masked.append([halves(jnp.where(which == c, mine, 0.0)) for c in range(per)])

    def filtered(table_ref, x, parts):
        for h in range(2):
            total = None
            for c in range(per):
                at = half * (3 * c + 1 - h)
                rows = table_ref[x, :, at : at + height]
                for k in parts:
                    part = dot(rows, masked[x][c][k], ((1,), (0,)))
                    total = part if total is None else total + part
            yield slice(half * h, half * (h + 1)), slice(LANES * x, LANES * (x + 1)), total

    for x in range(quarters):
        for at, lanes, total in filtered(high_ref, x, (0, 1)):
            vertical_ref[at, lanes] = total
    low_copy.wait()
    for x in range(quarters):
        for at, lanes, total in filtered(low_ref, x, (0,)):
            vertical_ref[at, lanes] += total
    mix_copy.wait()
    mixed = dot_of_halves(halves(vertical_ref[...]), (mix_ref[0], mix_ref[1]), ((1,), (0,)))
    for x in range(quarters):
        for s in range(sources):
            at = strip * (quarters * s + x)
            out_ref[at : at + strip, :] = mixed[strip * s : strip * (s + 1), LANES * x : LANES * (x + 1)]


def unpack_kernel(in_ref, out_hbm, out_ref, strip_ref, sent):
    channels, rows, cols = out_ref.shape
    tiles = cols // LANES
    quarters = strip_ref.shape[0]
    for q in range(quarters):
        for t in range(tiles):
            at = rows * (quarters * t + q)
            strip_ref[q, rows * t : rows * (t + 1), :] = in_ref[at : at + rows, :]
    parts = [strip_ref[q] for q in range(quarters)]
    copies = [pltpu.make_async_copy(out_ref.at[o], out_hbm.at[o], sent.at[o]) for o in range(channels)]
    for o in range(channels):
        (value,) = blocks_transposed(parts, [o])
        for t in range(tiles):
            out_ref[o, :, LANES * t : LANES * (t + 1)] = value[rows * t : rows * (t + 1), :]
        copies[o].start()
    for copy in copies:
        copy.wait()


def in_vmem(value):
    return pltpu.with_memory_space_constraint(value, pltpu.VMEM)


def in_hbm(value):
    return pltpu.with_memory_space_constraint(value, pltpu.HBM)


def on_device(slide_region, row_taps, column_taps, channel_mix):
    channels, rows, cols = slide_region.shape
    bands = lax.axis_size(BAND)
    quarters = lax.axis_size("chan")
    height = rows * bands
    everyone = bands * quarters
    all_channels = column_taps.shape[0]
    per = all_channels // quarters
    flat = pltpu.VMEM((everyone * rows, LANES), F32)
    scratch = pltpu.VMEM
    lanes = quarters * LANES

    packed = pl.pallas_call(
        across_kernel,
        out_shape=flat,
        in_specs=[IN_HBM, pl.BlockSpec()],
        out_specs=IN_VMEM,
        scratch_shapes=[
            scratch((channels, rows, cols), F32),
            scratch((channels, 4 * LANES), F32),
            scratch((channels, rows * (cols // (2 * LANES)), 4 * LANES), F32),
            pltpu.SemaphoreType.DMA((channels,)),
        ],
        compiler_params=SMALL,
        name="across",
    )(in_hbm(slide_region), in_hbm(row_taps))
    table = (quarters, height // 2, per * (height // 2) * 3)
    high, low, wide_mix = pl.pallas_call(
        tables_kernel,
        out_shape=(
            pltpu.VMEM(table, BF16),
            pltpu.HBM(table, BF16),
            pltpu.HBM((2, lanes, lanes), BF16),
        ),
        in_specs=[pl.BlockSpec(), pl.BlockSpec()],
        out_specs=[IN_VMEM, pl.BlockSpec(), pl.BlockSpec()],
        scratch_shapes=[scratch((all_channels, 4 * LANES), F32)],
        compiler_params=SMALL,
        name="tables",
    )(in_hbm(column_taps), in_hbm(channel_mix))

    def exchanged(value):
        parts = value.reshape(everyone, rows, LANES)
        moved = lax.all_to_all(parts, EVERYONE, 0, 0, tiled=True)
        return in_vmem(moved.reshape(value.shape))

    mixed = pl.pallas_call(
        lambda *refs: vertical_kernel(rows, *refs),
        out_shape=flat,
        in_specs=[IN_VMEM, IN_VMEM, IN_HBM, IN_HBM],
        out_specs=IN_VMEM,
        scratch_shapes=[
            scratch((quarters, height, LANES), F32),
            scratch((height, lanes), F32),
            scratch(table, BF16),
            scratch((2, lanes, lanes), BF16),
            pltpu.SemaphoreType.DMA((2,)),
        ],
        compiler_params=SMALL,
        name="vertical",
    )(exchanged(packed), in_vmem(high), in_hbm(low), in_hbm(wide_mix))
    return pl.pallas_call(
        unpack_kernel,
        out_shape=jax.ShapeDtypeStruct((channels, rows, cols), F32),
        in_specs=[IN_VMEM],
        out_specs=IN_HBM,
        scratch_shapes=[
            scratch((channels, rows, cols), F32),
            scratch((quarters, rows * (cols // LANES), LANES), F32),
            pltpu.SemaphoreType.DMA((channels,)),
        ],
        compiler_params=SMALL,
        name="unpack",
    )(exchanged(mixed))


def solution(mesh):
    bands = mesh.shape["band"]
    split = Mesh(
        mesh.devices.reshape(mesh.shape["groups"], bands // 2, 2, mesh.shape["chan"]),
        ("groups", "band_0", "band_1", "chan"),
    )
    in_specs = (P("chan", GROUPS_BAND, None), P("chan", None), P(), P())
    out_specs = P("chan", GROUPS_BAND, None)
    return jax.shard_map(
        on_device, mesh=split, in_specs=in_specs, out_specs=out_specs, check_vma=False
    )
```

```python
import jax
import jax.numpy as jnp
from jax import lax
from jax.experimental import pallas as pl
from jax.experimental.pallas import tpu as pltpu
from jax.sharding import Mesh
from jax.sharding import PartitionSpec as P

BAND = ("band_0", "band_1")
GROUPS_BAND = ("groups", "band_0", "band_1")
EVERYONE = ("band_0", "band_1", "chan")
LANES = 128
SUBLANES = 8
F32 = jnp.float32
BF16 = jnp.bfloat16
IN_VMEM = pl.BlockSpec(memory_space=pltpu.VMEM)
IN_HBM = pl.BlockSpec(memory_space=pltpu.HBM)
SMALL = pltpu.CompilerParams(vmem_limit_bytes=16 * 1024 * 1024)


def halves(value):
    high = value.astype(BF16)
    return high, (value - high.astype(F32)).astype(BF16)


def dot(a, b, dims):
    return lax.dot_general(a, b, (dims, ((), ())), preferred_element_type=F32)


def dot_of_halves(a, b, dims):
    (a_high, a_low), (b_high, b_low) = a, b
    return dot(a_high, b_high, dims) + (dot(a_high, b_low, dims) + dot(a_low, b_high, dims))


def lane_block(shape, width):
    return lax.broadcasted_iota(jnp.int32, shape, len(shape) - 1) // width


def blocks_transposed(parts, wanted):
    width = LANES // len(parts)
    which = lane_block(parts[0].shape, width)
    out = []
    for b in wanted:
        total = None
        for a, part in enumerate(parts):
            shift = (width * (a - b)) % LANES
            moved = pltpu.roll(part, shift, axis=1) if shift else part
            total = moved if total is None else jnp.where(which == a, moved, total)
        out.append(total)
    return out


def shifted_copies(taps_row, rows, size, first):
    wide = jnp.broadcast_to(taps_row, (rows, size))
    return pltpu.roll(wide, first % size, axis=1, stride=1, stride_axis=0)


def across_kernel(rows, x_hbm, taps_ref, out_ref, x_ref, padded_ref, arrived):
    channels, body = x_hbm.shape[0:2]
    length = taps_ref.shape[1]
    copies = [
        pltpu.make_async_copy(x_hbm.at[c], x_ref.at[c, pl.ds(SUBLANES, body), :], arrived.at[c])
        for c in range(channels)
    ]
    for copy in copies:
        copy.start()
    padded_ref[...] = jnp.zeros(padded_ref.shape, F32)
    padded_ref[:, 0:length] = taps_ref[...]
    edge = jnp.zeros((SUBLANES, LANES), F32)
    filtered = []
    for c in range(channels):
        x_ref[c, 0:SUBLANES, :] = edge
        x_ref[c, SUBLANES + body : 2 * SUBLANES + body, :] = edge
        rolled = shifted_copies(padded_ref[c : c + 1, :], LANES, padded_ref.shape[1], 0)
        table = halves(rolled[:, 0 : 3 * LANES])
        copies[c].wait()
        first = SUBLANES - rows
        near = [x_ref[c, first + rows * k : first + rows * k + body, :] for k in range(3)]
        filtered.append(dot_of_halves(halves(jnp.concatenate(near, axis=1)), table, ((1,), (1,))))
    packed = blocks_transposed(filtered, range(channels))
    for q, value in enumerate(packed):
        for t in range(body // rows):
            at = rows * (channels * t + q)
            out_ref[at : at + rows, :] = value[rows * t : rows * (t + 1), :]


def tables_kernel(taps_ref, mix_ref, high_ref, low_ref, wide_mix_ref, padded_ref):
    channels, length = taps_ref.shape
    quarters, half = high_ref.shape[0:2]
    margin = (length - 1) // 2
    padded_ref[...] = jnp.zeros(padded_ref.shape, F32)
    padded_ref[:, 0:length] = taps_ref[...]
    per = channels // quarters
    for c in range(channels):
        rolled = shifted_copies(padded_ref[c : c + 1, :], half, padded_ref.shape[1], half - margin)
        high, low = halves(rolled[:, 0 : 3 * half])
        at = 3 * half * (c % per)
        high_ref[c // per, :, at : at + 3 * half] = high
        low_ref[c // per, :, at : at + 3 * half] = low
    n = wide_mix_ref.shape[1]
    width = n // channels
    spread = (
        lax.broadcasted_iota(jnp.int32, (n, channels), 0) // width
        == lax.broadcasted_iota(jnp.int32, (n, channels), 1)
    ).astype(F32)
    precise = dict(precision=lax.Precision.HIGHEST, preferred_element_type=F32)
    tall = lax.dot_general(spread, mix_ref[...], (((1,), (1,)), ((), ())), **precise)
    wide = lax.dot_general(tall, spread, (((1,), (1,)), ((), ())), **precise)
    same = (
        lax.broadcasted_iota(jnp.int32, (n, n), 0) % width
        == lax.broadcasted_iota(jnp.int32, (n, n), 1) % width
    )
    wide_mix_ref[0], wide_mix_ref[1] = halves(jnp.where(same, wide, 0.0))


def vertical_kernel(
    strip, in_ref, high_ref, low_hbm, mix_ref, out_ref, gathered_ref, vertical_ref, low_ref, arrived
):
    quarters, height = gathered_ref.shape[0:2]
    half = height // 2
    per = high_ref.shape[2] // (3 * half)
    sources = height // strip
    low_copy = pltpu.make_async_copy(low_hbm, low_ref, arrived)
    low_copy.start()
    which = lane_block((height, LANES), LANES // per)
    masked = []
    for x in range(quarters):
        for s in range(sources):
            at = strip * (quarters * s + x)
            gathered_ref[x, strip * s : strip * (s + 1), :] = in_ref[at : at + strip, :]
        mine = gathered_ref[x]
        masked.append([halves(jnp.where(which == c, mine, 0.0)) for c in range(per)])

    def filtered(table_ref, x, parts):
        for h in range(2):
            total = None
            for c in range(per):
                at = half * (3 * c + 1 - h)
                rows = table_ref[x, :, at : at + height]
                for k in parts:
                    part = dot(rows, masked[x][c][k], ((1,), (0,)))
                    total = part if total is None else total + part
            yield slice(half * h, half * (h + 1)), slice(LANES * x, LANES * (x + 1)), total

    for x in range(quarters):
        for at, lanes, total in filtered(high_ref, x, (0, 1)):
            vertical_ref[at, lanes] = total
    mixed = dot_of_halves(halves(vertical_ref[...]), (mix_ref[0], mix_ref[1]), ((1,), (0,)))
    low_copy.wait()
    for x in range(quarters):
        for at, lanes, total in filtered(low_ref, x, (0,)):
            vertical_ref[at, lanes] = total
    mixed = mixed + dot(vertical_ref[...].astype(BF16), mix_ref[0], ((1,), (0,)))
    for x in range(quarters):
        for s in range(sources):
            at = strip * (quarters * s + x)
            out_ref[at : at + strip, :] = mixed[strip * s : strip * (s + 1), LANES * x : LANES * (x + 1)]


def unpack_kernel(rows, in_ref, out_hbm, out_ref, strip_ref, sent):
    channels, body = out_ref.shape[0:2]
    quarters = strip_ref.shape[0]
    for q in range(quarters):
        for t in range(body // rows):
            at = rows * (quarters * t + q)
            strip_ref[q, rows * t : rows * (t + 1), :] = in_ref[at : at + rows, :]
    parts = [strip_ref[q] for q in range(quarters)]
    copies = [pltpu.make_async_copy(out_ref.at[o], out_hbm.at[o], sent.at[o]) for o in range(channels)]
    for o in range(channels):
        (out_ref[o],) = blocks_transposed(parts, [o])
        copies[o].start()
    for copy in copies:
        copy.wait()


def in_vmem(value):
    return pltpu.with_memory_space_constraint(value, pltpu.VMEM)


def in_hbm(value):
    return pltpu.with_memory_space_constraint(value, pltpu.HBM)


def on_device(slide_region, row_taps, column_taps, channel_mix):
    channels, rows, cols = slide_region.shape
    bands = lax.axis_size(BAND)
    quarters = lax.axis_size("chan")
    height = rows * bands
    everyone = bands * quarters
    all_channels = column_taps.shape[0]
    per = all_channels // quarters
    flat = pltpu.VMEM((everyone * rows, LANES), F32)
    scratch = pltpu.VMEM
    lanes = quarters * LANES

    tiles = cols // LANES
    stacked = (channels, tiles * rows, LANES)
    by_tile = slide_region.reshape(channels, rows, tiles, LANES).transpose(0, 2, 1, 3).reshape(stacked)
    packed = pl.pallas_call(
        lambda *refs: across_kernel(rows, *refs),
        out_shape=flat,
        in_specs=[IN_HBM, pl.BlockSpec()],
        out_specs=IN_VMEM,
        scratch_shapes=[
            scratch((channels, tiles * rows + 2 * SUBLANES, LANES), F32),
            scratch((channels, 4 * LANES), F32),
            pltpu.SemaphoreType.DMA((channels,)),
        ],
        compiler_params=SMALL,
        name="across",
    )(in_hbm(by_tile), in_hbm(row_taps))
    table = (quarters, height // 2, per * (height // 2) * 3)
    high, low, wide_mix = pl.pallas_call(
        tables_kernel,
        out_shape=(
            pltpu.VMEM(table, BF16),
            pltpu.HBM(table, BF16),
            pltpu.VMEM((2, lanes, lanes), BF16),
        ),
        in_specs=[pl.BlockSpec(), pl.BlockSpec()],
        out_specs=[IN_VMEM, pl.BlockSpec(), IN_VMEM],
        scratch_shapes=[scratch((all_channels, 4 * LANES), F32)],
        compiler_params=SMALL,
        name="tables",
    )(in_hbm(column_taps), in_hbm(channel_mix))

    def exchanged(value):
        parts = value.reshape(everyone, rows, LANES)
        moved = lax.all_to_all(parts, EVERYONE, 0, 0, tiled=True)
        return in_vmem(moved.reshape(value.shape))

    mixed = pl.pallas_call(
        lambda *refs: vertical_kernel(rows, *refs),
        out_shape=flat,
        in_specs=[IN_VMEM, IN_VMEM, IN_HBM, IN_VMEM],
        out_specs=IN_VMEM,
        scratch_shapes=[
            scratch((quarters, height, LANES), F32),
            scratch((height, lanes), F32),
            scratch(table, BF16),
            pltpu.SemaphoreType.DMA,
        ],
        compiler_params=SMALL,
        name="vertical",
    )(exchanged(packed), in_vmem(high), in_hbm(low), in_vmem(wide_mix))
    joined = pl.pallas_call(
        lambda *refs: unpack_kernel(rows, *refs),
        out_shape=pltpu.HBM(stacked, F32),
        in_specs=[IN_VMEM],
        out_specs=IN_HBM,
        scratch_shapes=[
            scratch(stacked, F32),
            scratch((quarters, tiles * rows, LANES), F32),
            pltpu.SemaphoreType.DMA((channels,)),
        ],
        compiler_params=SMALL,
        name="unpack",
    )(exchanged(mixed))
    return joined.reshape(channels, tiles, rows, LANES).transpose(0, 2, 1, 3).reshape(channels, rows, cols)


def solution(mesh):
    bands = mesh.shape["band"]
    split = Mesh(
        mesh.devices.reshape(mesh.shape["groups"], bands // 2, 2, mesh.shape["chan"]),
        ("groups", "band_0", "band_1", "chan"),
    )
    in_specs = (P("chan", GROUPS_BAND, None), P("chan", None), P(), P())
    out_specs = P("chan", GROUPS_BAND, None)
    return jax.shard_map(
        on_device, mesh=split, in_specs=in_specs, out_specs=out_specs, check_vma=False
    )
```

```python
import jax
import jax.numpy as jnp
from jax import lax
from jax.experimental import pallas as pl
from jax.experimental.pallas import tpu as pltpu
from jax.sharding import Mesh
from jax.sharding import PartitionSpec as P

BAND = ("band_0", "band_1")
GROUPS_BAND = ("groups", "band_0", "band_1")
EVERYONE = ("band_0", "band_1", "chan")
LANES = 128
SUBLANES = 8
PARTS = 1
F32 = jnp.float32
BF16 = jnp.bfloat16
IN_VMEM = pl.BlockSpec(memory_space=pltpu.VMEM)
IN_HBM = pl.BlockSpec(memory_space=pltpu.HBM)
SMALL = pltpu.CompilerParams(vmem_limit_bytes=16 * 1024 * 1024)


def halves(value):
    high = value.astype(BF16)
    return high, (value - high.astype(F32)).astype(BF16)


def dot(a, b, dims):
    return lax.dot_general(a, b, (dims, ((), ())), preferred_element_type=F32)


def dot_of_halves(a, b, dims):
    (a_high, a_low), (b_high, b_low) = a, b
    return dot(a_high, b_high, dims) + (dot(a_high, b_low, dims) + dot(a_low, b_high, dims))


def lane_block(shape, width):
    return lax.broadcasted_iota(jnp.int32, shape, len(shape) - 1) // width


def blocks_transposed(parts, wanted):
    width = LANES // len(parts)
    which = lane_block(parts[0].shape, width)
    out = []
    for b in wanted:
        total = None
        for a, part in enumerate(parts):
            shift = (width * (a - b)) % LANES
            moved = pltpu.roll(part, shift, axis=1) if shift else part
            total = moved if total is None else jnp.where(which == a, moved, total)
        out.append(total)
    return out


def shifted_copies(taps_row, rows, size, first):
    wide = jnp.broadcast_to(taps_row, (rows, size))
    return pltpu.roll(wide, first % size, axis=1, stride=1, stride_axis=0)


def across_kernel(rows, x_hbm, taps_ref, out_hbm, x_ref, padded_ref, out_ref, arrived, out_copies):
    channels, body = x_hbm.shape[0:2]
    length = taps_ref.shape[1]
    parts = out_copies.shape[0]
    size = body // parts
    ends = [0] + [size * (h + 1) + SUBLANES for h in range(parts - 1)] + [body]
    copies = [
        pltpu.make_async_copy(
            x_hbm.at[:, pl.ds(ends[h], ends[h + 1] - ends[h]), :],
            x_ref.at[:, pl.ds(SUBLANES + ends[h], ends[h + 1] - ends[h]), :],
            arrived.at[h],
        )
        for h in range(parts)
    ]
    for copy in copies:
        copy.start()
    padded_ref[...] = jnp.zeros(padded_ref.shape, F32)
    padded_ref[:, 0:length] = taps_ref[...]
    edge = jnp.zeros((SUBLANES, LANES), F32)
    tables = []
    for c in range(channels):
        x_ref[c, 0:SUBLANES, :] = edge
        x_ref[c, SUBLANES + body : 2 * SUBLANES + body, :] = edge
        rolled = shifted_copies(padded_ref[c : c + 1, :], LANES, padded_ref.shape[1], 0)
        tables.append(halves(rolled[:, 0 : 3 * LANES]))
    first = SUBLANES - rows
    leaving = []
    for h in range(parts):
        filtered = []
        copies[h].wait()
        for c in range(channels):
            near = [x_ref[c, pl.ds(first + rows * k + size * h, size), :] for k in range(3)]
            filtered.append(dot_of_halves(halves(jnp.concatenate(near, axis=1)), tables[c], ((1,), (1,))))
        packed = blocks_transposed(filtered, range(channels))
        for q, value in enumerate(packed):
            for t in range(size // rows):
                at = rows * (channels * t + q) + channels * size * h
                out_ref[at : at + rows, :] = value[rows * t : rows * (t + 1), :]
        piece = pl.ds(channels * size * h, channels * size)
        leaving.append(pltpu.make_async_copy(out_ref.at[piece], out_hbm.at[piece], out_copies.at[h]))
        leaving[-1].start()
    for copy in leaving:
        copy.wait()


def tables_kernel(taps_ref, mix_ref, high_ref, low_ref, wide_mix_ref, padded_ref):
    channels, length = taps_ref.shape
    quarters, half = high_ref.shape[0:2]
    margin = (length - 1) // 2
    padded_ref[...] = jnp.zeros(padded_ref.shape, F32)
    padded_ref[:, 0:length] = taps_ref[...]
    per = channels // quarters
    for c in range(channels):
        rolled = shifted_copies(padded_ref[c : c + 1, :], half, padded_ref.shape[1], half - margin)
        high, low = halves(rolled[:, 0 : 3 * half])
        at = 3 * half * (c % per)
        high_ref[c // per, :, at : at + 3 * half] = high
        low_ref[c // per, :, at : at + 3 * half] = low
    n = wide_mix_ref.shape[1]
    width = n // channels
    spread = (
        lax.broadcasted_iota(jnp.int32, (n, channels), 0) // width
        == lax.broadcasted_iota(jnp.int32, (n, channels), 1)
    ).astype(F32)
    precise = dict(precision=lax.Precision.HIGHEST, preferred_element_type=F32)
    tall = lax.dot_general(spread, mix_ref[...], (((1,), (1,)), ((), ())), **precise)
    wide = lax.dot_general(tall, spread, (((1,), (1,)), ((), ())), **precise)
    same = (
        lax.broadcasted_iota(jnp.int32, (n, n), 0) % width
        == lax.broadcasted_iota(jnp.int32, (n, n), 1) % width
    )
    wide_mix_ref[0], wide_mix_ref[1] = halves(jnp.where(same, wide, 0.0))


def vertical_kernel(
    strip, in_ref, high_ref, low_hbm, mix_ref, out_ref, gathered_ref, vertical_ref, low_ref, arrived
):
    quarters, height = gathered_ref.shape[0:2]
    half = height // 2
    per = high_ref.shape[2] // (3 * half)
    sources = height // strip
    low_copy = pltpu.make_async_copy(low_hbm, low_ref, arrived)
    low_copy.start()
    which = lane_block((height, LANES), LANES // per)
    masked = []
    for x in range(quarters):
        for s in range(sources):
            at = strip * (quarters * s + x)
            gathered_ref[x, strip * s : strip * (s + 1), :] = in_ref[at : at + strip, :]
        mine = gathered_ref[x]
        masked.append([halves(jnp.where(which == c, mine, 0.0)) for c in range(per)])

    def filtered(table_ref, x, parts):
        for h in range(2):
            total = None
            for c in range(per):
                at = half * (3 * c + 1 - h)
                rows = table_ref[x, :, at : at + height]
                for k in parts:
                    part = dot(rows, masked[x][c][k], ((1,), (0,)))
                    total = part if total is None else total + part
            yield slice(half * h, half * (h + 1)), slice(LANES * x, LANES * (x + 1)), total

    for x in range(quarters):
        for at, lanes, total in filtered(high_ref, x, (0, 1)):
            vertical_ref[at, lanes] = total
    mixed = dot_of_halves(halves(vertical_ref[...]), (mix_ref[0], mix_ref[1]), ((1,), (0,)))
    low_copy.wait()
    for x in range(quarters):
        for at, lanes, total in filtered(low_ref, x, (0,)):
            vertical_ref[at, lanes] = total
    mixed = mixed + dot(vertical_ref[...].astype(BF16), mix_ref[0], ((1,), (0,)))
    for x in range(quarters):
        for s in range(sources):
            at = strip * (quarters * s + x)
            out_ref[at : at + strip, :] = mixed[strip * s : strip * (s + 1), LANES * x : LANES * (x + 1)]


def unpack_kernel(rows, in_ref, out_hbm, out_ref, strip_ref, sent):
    channels, body = out_ref.shape[0:2]
    quarters = strip_ref.shape[0]
    for q in range(quarters):
        for t in range(body // rows):
            at = rows * (quarters * t + q)
            strip_ref[q, rows * t : rows * (t + 1), :] = in_ref[at : at + rows, :]
    parts = [strip_ref[q] for q in range(quarters)]
    copies = [pltpu.make_async_copy(out_ref.at[o], out_hbm.at[o], sent.at[o]) for o in range(channels)]
    for o in range(channels):
        (out_ref[o],) = blocks_transposed(parts, [o])
        copies[o].start()
    for copy in copies:
        copy.wait()


def in_vmem(value):
    return pltpu.with_memory_space_constraint(value, pltpu.VMEM)


def in_hbm(value):
    return pltpu.with_memory_space_constraint(value, pltpu.HBM)


def on_device(slide_region, row_taps, column_taps, channel_mix):
    channels, rows, cols = slide_region.shape
    bands = lax.axis_size(BAND)
    quarters = lax.axis_size("chan")
    height = rows * bands
    everyone = bands * quarters
    all_channels = column_taps.shape[0]
    per = all_channels // quarters
    flat = pltpu.VMEM((everyone * rows, LANES), F32)
    scratch = pltpu.VMEM
    lanes = quarters * LANES

    tiles = cols // LANES
    stacked = (channels, tiles * rows, LANES)
    by_tile = slide_region.reshape(channels, rows, tiles, LANES).transpose(0, 2, 1, 3).reshape(stacked)
    packed = pl.pallas_call(
        lambda *refs: across_kernel(rows, *refs),
        out_shape=pltpu.HBM(flat.shape, F32),
        in_specs=[IN_HBM, pl.BlockSpec()],
        out_specs=IN_HBM,
        scratch_shapes=[
            scratch((channels, tiles * rows + 2 * SUBLANES, LANES), F32),
            scratch((channels, 4 * LANES), F32),
            scratch(flat.shape, F32),
            pltpu.SemaphoreType.DMA((PARTS,)),
            pltpu.SemaphoreType.DMA((PARTS,)),
        ],
        compiler_params=SMALL,
        name="across",
    )(in_hbm(by_tile), in_hbm(row_taps))
    table = (quarters, height // 2, per * (height // 2) * 3)
    high, low, wide_mix = pl.pallas_call(
        tables_kernel,
        out_shape=(
            pltpu.VMEM(table, BF16),
            pltpu.HBM(table, BF16),
            pltpu.VMEM((2, lanes, lanes), BF16),
        ),
        in_specs=[pl.BlockSpec(), pl.BlockSpec()],
        out_specs=[IN_VMEM, pl.BlockSpec(), IN_VMEM],
        scratch_shapes=[scratch((all_channels, 4 * LANES), F32)],
        compiler_params=SMALL,
        name="tables",
    )(in_hbm(column_taps), in_hbm(channel_mix))

    def exchanged(value):
        parts = value.reshape(everyone, rows, LANES)
        moved = lax.all_to_all(parts, EVERYONE, 0, 0, tiled=True)
        return in_vmem(moved.reshape(value.shape))

    mixed = pl.pallas_call(
        lambda *refs: vertical_kernel(rows, *refs),
        out_shape=flat,
        in_specs=[IN_VMEM, IN_VMEM, IN_HBM, IN_VMEM],
        out_specs=IN_VMEM,
        scratch_shapes=[
            scratch((quarters, height, LANES), F32),
            scratch((height, lanes), F32),
            scratch(table, BF16),
            pltpu.SemaphoreType.DMA,
        ],
        compiler_params=SMALL,
        name="vertical",
    )(exchanged(packed), in_vmem(high), in_hbm(low), in_vmem(wide_mix))
    joined = pl.pallas_call(
        lambda *refs: unpack_kernel(rows, *refs),
        out_shape=pltpu.HBM(stacked, F32),
        in_specs=[IN_VMEM],
        out_specs=IN_HBM,
        scratch_shapes=[
            scratch(stacked, F32),
            scratch((quarters, tiles * rows, LANES), F32),
            pltpu.SemaphoreType.DMA((channels,)),
        ],
        compiler_params=SMALL,
        name="unpack",
    )(exchanged(mixed))
    return joined.reshape(channels, tiles, rows, LANES).transpose(0, 2, 1, 3).reshape(channels, rows, cols)


def solution(mesh):
    bands = mesh.shape["band"]
    split = Mesh(
        mesh.devices.reshape(mesh.shape["groups"], bands // 2, 2, mesh.shape["chan"]),
        ("groups", "band_0", "band_1", "chan"),
    )
    in_specs = (P("chan", GROUPS_BAND, None), P("chan", None), P(), P())
    out_specs = P("chan", GROUPS_BAND, None)
    return jax.shard_map(
        on_device, mesh=split, in_specs=in_specs, out_specs=out_specs, check_vma=False
    )
```
